32 devices in a mesh: pw: 8 (over y, x, core), mode: 4 (over z).
Axes of the slice: x: 2, y: 2, z: 4, core: 2. Of those that a mesh axis runs over, the one named last changes fastest.
Arguments:
- wave_coeffs: bfloat16 [2, 192, 32768], P(None, 'mode', 'pw'), may hold values from -0.03125 to 0.03125
- sphere_map: int32 [32768], P('pw'), may hold values from 0 to 32768, as said below
- wave_kq: bfloat16 [192, 64, 64, 128], P(None, 'pw'), may hold values from -6 to 6
- potential: bfloat16 [4, 64, 64, 128], P('mode', 'pw'), may hold values from -6 to 6
- shift_map: int32 [3], replicated, may hold values from -1 to 1
Outputs:
- coupling: float32 [192, 2, 192, 4], P('pw', None, None, 'mode')
The draws below stay inside these ranges and needn't reach their ends.
Inputs may be any that keep to these rules, and one draw needn't show every extreme that they name: `sphere_map`: entries 4096 * p to 4096 * (p + 1) - 1 belong to pw shard p, whose grid planes are g1 = p * 64 / 8 and the next ones. A live entry is a cell of that shard's planes, numbered (local plane * 64 + g2) * 64 + g3, and live entries of one shard are distinct; the value 32768 marks an unused slot. Some shards use all their slots.
All inputs are finite; a program needn't handle non-finite values.
Results may differ from the reference program's by a relative error of at most 0.023.
Values may be sent and summed in bfloat16 or wider, within the bound.
No kernel may reach another device: no remote copies, remote signals or barrier semaphores. Data moves between devices by JAX's collectives and lax.ppermute only.
A program may use at most 256 MiB of HBM per device.

```python
import math
import jax
import jax.numpy as jnp
from jax import lax

NG = 64
BANDS = 192
NPW = 32768
MODES = 4
PW_DEV = 4096
SLAB = 32768


def draw_sphere_map(key, part):
    shards = NPW // PW_DEV
    offset = jax.random.randint(jax.random.fold_in(key, 7), (), 0, 4)

    def one_shard(shard_id):
        shard_key = jax.random.fold_in(key, shard_id + 11)
        cell_ids = jax.random.permutation(jax.random.fold_in(shard_key, 1), SLAB)[:PW_DEV]
        order_ids = jax.random.permutation(jax.random.fold_in(shard_key, 2), PW_DEV)
        dropped = jax.random.randint(jax.random.fold_in(shard_key, 3), (), 0, PW_DEV // 2 + 1)
        dropped = jnp.where((shard_id + offset) % 4 == 0, 0, dropped)
        live_mask = order_ids < PW_DEV - dropped
        return jnp.where(live_mask, cell_ids, SLAB).astype(jnp.int32)
    return jax.vmap(one_shard)(jnp.arange(shards, dtype=jnp.int32)).reshape(NPW)


def steps_of(own_key, shape, cuts, smallest, largest):
    def one(axis_at, parts):
        heights = jax.random.uniform(jax.random.fold_in(jax.random.fold_in(own_key, 6), axis_at), (parts,), jnp.float32, smallest / len(cuts), largest / len(cuts))
        return jnp.repeat(jnp.exp(heights), shape[axis_at] // parts).reshape((-1,) + (1,) * (len(shape) - axis_at - 1))

    factor_of = one(*cuts[0])
    for cut in cuts[1:]:
        factor_of = factor_of * one(*cut)
    return factor_of


def noise(stream_key, dims, deviation, reach, cuts=(), held_as=jnp.bfloat16):
    gain = steps_of(stream_key, dims, cuts, -0.22, 0.18) if cuts else 1.0
    array = jax.random.normal(stream_key, dims, jnp.float32) * deviation * gain
    return jnp.minimum(jnp.maximum(array, -reach), reach).astype(held_as)


def setup_inputs(seed: int = 0) -> dict:
    key_list = jax.random.split(jax.random.key(seed), 6)
    return {
        "wave_coeffs": noise(key_list[0], (2, BANDS, NPW), NPW ** -0.5, 0.03125, ((1, 4), (2, 8))),
        "sphere_map": draw_sphere_map(jax.random.fold_in(key_list[5], 71), 0),
        "wave_kq": noise(key_list[2], (BANDS, NG, NG, 2 * NG), 1.0, 6.0, ((1, 8),)),
        "potential": noise(key_list[3], (MODES, NG, NG, 2 * NG), 1.0, 6.0, ((0, 4), (1, 8))),
        "shift_map": jax.random.randint(key_list[4], (3,), -1, 2).astype(jnp.int32),
    }


HIGHEST_PREC = lax.Precision.HIGHEST


def stored(value):
    return lax.optimization_barrier(value.astype(jnp.bfloat16)).astype(jnp.float32)


def dft_parts():
    positions = jnp.arange(NG, dtype=jnp.int32)
    angles = ((positions[:, None] * positions[None, :]) % NG).astype(jnp.float32) * (2.0 * math.pi / NG)
    return stored(jnp.cos(angles)), stored(jnp.sin(angles))


def along_last(real_part, imag_part, cosine, sine_table):
    out_real = jnp.matmul(real_part, cosine, precision=HIGHEST_PREC) - jnp.matmul(imag_part, sine_table, precision=HIGHEST_PREC)
    out_imag = jnp.matmul(real_part, sine_table, precision=HIGHEST_PREC) + jnp.matmul(imag_part, cosine, precision=HIGHEST_PREC)
    return stored(out_real), stored(out_imag)


def reference(wave_coeffs, sphere_map, wave_kq, potential, shift_map):
    cosine, sine_table = dft_parts()
    slot_ids = jnp.arange(NPW, dtype=jnp.int32)
    target = jnp.where(sphere_map < SLAB, (slot_ids // PW_DEV) * SLAB + sphere_map, NG ** 3).astype(jnp.int32)

    def place_grid(component):
        flat_grid = jnp.zeros((BANDS, NG ** 3 + 1), jnp.float32).at[:, target].add(component.astype(jnp.float32))
        return flat_grid[:, :NG ** 3].reshape(BANDS, NG, NG, NG)

    grid_real = place_grid(wave_coeffs[0])
    grid_imag = place_grid(wave_coeffs[1])
    section_real, section_imag = along_last(grid_real, grid_imag, cosine, sine_table)
    section_real, section_imag = along_last(jnp.transpose(section_real, (0, 1, 3, 2)), jnp.transpose(section_imag, (0, 1, 3, 2)), cosine, sine_table)
    k_real, k_imag = along_last(jnp.transpose(section_real, (0, 3, 2, 1)), jnp.transpose(section_imag, (0, 3, 2, 1)), cosine, sine_table)

    grid_axis = jnp.arange(NG, dtype=jnp.int32)
    phase_sum = (shift_map[0] * grid_axis[None, None, :] + shift_map[1] * grid_axis[:, None, None] + shift_map[2] * grid_axis[None, :, None]) % NG
    angles = phase_sum.astype(jnp.float32) * (2.0 * math.pi / NG)
    phase_cos = jnp.cos(angles)
    phase_sin = jnp.sin(angles)
    pot_real = potential[..., :NG].astype(jnp.float32)
    pot_imag = potential[..., NG:].astype(jnp.float32)
    phase_real = pot_real * phase_cos + pot_imag * phase_sin
    phase_imag = pot_imag * phase_cos - pot_real * phase_sin

    kq_real = wave_kq[..., :NG].astype(jnp.float32).reshape(BANDS, -1)
    kq_imag = wave_kq[..., NG:].astype(jnp.float32).reshape(BANDS, -1)
    kq_joined = jnp.concatenate([kq_real, kq_imag], 1)
    scale_factor = float(NG) ** -1.5

    def one_mode(mode_pair):
        mode_real, mode_imag = mode_pair
        weight_real = stored(mode_real[None] * k_real - mode_imag[None] * k_imag).reshape(BANDS, -1)
        weight_imag = stored(mode_real[None] * k_imag + mode_imag[None] * k_real).reshape(BANDS, -1)
        g_real = jnp.matmul(kq_joined, jnp.concatenate([weight_real, weight_imag], 1).T, precision=HIGHEST_PREC)
        g_imag = jnp.matmul(kq_joined, jnp.concatenate([weight_imag, -weight_real], 1).T, precision=HIGHEST_PREC)
        return jnp.stack([g_real, g_imag]) * scale_factor

    per_mode = lax.map(one_mode, (phase_real, phase_imag))
    return jnp.transpose(per_mode, (2, 1, 3, 0))
```

```python
import functools
import math

import jax
import jax.numpy as jnp
from jax import lax
from jax.experimental import pallas as pl
from jax.experimental.pallas import tpu as pltpu
from jax.sharding import PartitionSpec as P

def place_kernel(re_ref, im_ref, map_ref, ty_ref, l1_ref, h_ref, oht, wst, gt, *, ng, yc, planes, chunk):
    bands, slots = re_ref.shape
    half = wst.shape[0] // 2
    rows = planes * ng
    used = yc * bands
    if used < half:
        for c in range(2):
            wst[c * half + used:(c + 1) * half] = jnp.zeros((half - used, slots), jnp.bfloat16)
    for j in range(slots // chunk):
        sl = slice(j * chunk, (j + 1) * chunk)
        cells = map_ref[:, sl]
        key = (cells // (ng * ng)) * ng + cells % ng
        g2 = (cells // ng) % ng
        ohy = (lax.broadcasted_iota(jnp.int32, (ng, chunk), 0) == g2).astype(jnp.bfloat16)
        t = jnp.dot(ty_ref[...], ohy, preferred_element_type=jnp.float32)
        oht[:, sl] = (lax.broadcasted_iota(jnp.int32, (rows, chunk), 0) == key).astype(jnp.bfloat16)
        cr = re_ref[:, sl].astype(jnp.float32)
        ci = im_ref[:, sl].astype(jnp.float32)
        for y in range(yc):
            tr = t[y:y + 1]
            ti = t[yc + y:yc + y + 1]
            wst[y * bands:(y + 1) * bands, sl] = (cr * tr - ci * ti).astype(jnp.bfloat16)
            wst[half + y * bands:half + (y + 1) * bands, sl] = (cr * ti + ci * tr).astype(jnp.bfloat16)
    g = lax.dot_general(oht[...], wst[...], (((1,), (1,)), ((), ())), preferred_element_type=jnp.float32)
    gt[...] = g.astype(jnp.bfloat16)
    for p in range(planes):
        part = jnp.concatenate([gt[p * ng:(p + 1) * ng, :half], gt[p * ng:(p + 1) * ng, half:]], 0)
        res = jnp.dot(l1_ref[...], part, preferred_element_type=jnp.float32)
        for z in range(ng // 8):
            for t in range(half // 128):
                tile = slice(t * 128, (t + 1) * 128)
                h_ref[z, t, p * 8:(p + 1) * 8] = res[z * 8:(z + 1) * 8, tile]
                h_ref[z, t, (planes + p) * 8:(planes + p + 1) * 8] = res[ng + z * 8:ng + (z + 1) * 8, tile]

def place(re, im, m, ty, l1, *, ng, yc, planes, chunk=512):
    bands, slots = re.shape
    chunk = min(chunk, slots)
    half = -(-yc * bands // 128) * 128
    return pl.pallas_call(
        functools.partial(place_kernel, ng=ng, yc=yc, planes=planes, chunk=chunk),
        out_shape=jax.ShapeDtypeStruct((ng // 8, half // 128, 16 * planes, 128), jnp.float32),
        scratch_shapes=[pltpu.VMEM((planes * ng, slots), jnp.bfloat16), pltpu.VMEM((2 * half, slots), jnp.bfloat16), pltpu.VMEM((planes * ng, 2 * half), jnp.bfloat16)],
        compiler_params=pltpu.CompilerParams(vmem_limit_bytes=60 << 20),
        cost_estimate=pl.CostEstimate(flops=2 * planes * ng * slots * 2 * yc * bands, bytes_accessed=re.size * 4 + planes * ng * 2 * yc * bands * 4, transcendentals=0),
        name="place",
    )(re, im, m, ty, l1)

def couple_kernel(*refs, shards, yc, bands, modes, zb, scale):
    h_refs = refs[:shards]
    l2_ref, pr_ref, pi_ref, kq_ref, out_ref, psi, kf, kqs, wst, acc = refs[shards:]
    kq_bands = kq_ref.shape[0]
    tiles, part = h_refs[0].shape[1], h_refs[0].shape[2] // 8
    step = pl.program_id(0)

    @pl.when(step == 0)
    def _():
        acc[...] = jnp.zeros_like(acc)

    for z in range(zb):
        s = jnp.concatenate(
            [jnp.concatenate([h[z // 8, t, pl.ds(z % 8, part, stride=8), :] for h in h_refs], 0) for t in range(tiles)], 1
        ).astype(jnp.bfloat16)
        psi[z] = lax.dot_general(s, l2_ref[...], (((0,), (0,)), ((), ())), preferred_element_type=jnp.float32)
    lanes = lax.broadcasted_iota(jnp.int32, (1, 128), 1)
    sign = jnp.where(lanes < 64, -1.0, 1.0)
    pair = 2 * bands

    def column(y, carry):
        kv = kq_ref[:, y].astype(jnp.float32).reshape(kq_bands, zb // 8, 8, 128)
        for h in range(zb // 8):
            kf[h] = kv[:, h].reshape(kq_bands * 8, 128)
        for z in range(zb):
            kqs[:, z * 128:(z + 1) * 128] = kf[z // 8, pl.ds(z % 8, kq_bands, stride=8), :].astype(jnp.bfloat16)
            a = psi[z, pl.ds(pl.multiple_of(y * bands, 8), bands), :]
            b = pltpu.roll(a, 64, 1) * sign
            for nu in range(modes):
                pr = pr_ref[nu, y, z:z + 1, :]
                pi = pi_ref[nu, y, z:z + 1, :]
                wst[nu * pair:nu * pair + bands, z * 128:(z + 1) * 128] = (a * pr + b * pi).astype(jnp.bfloat16)
                wst[nu * pair + bands:(nu + 1) * pair, z * 128:(z + 1) * 128] = (a * pi - b * pr).astype(jnp.bfloat16)
        acc[...] += lax.dot_general(wst[...], kqs[...], (((1,), (1,)), ((), ())), preferred_element_type=jnp.float32)
        return carry

    lax.fori_loop(0, yc, column, 0)

    @pl.when(step == pl.num_programs(0) - 1)
    def _():
        t = acc[...].T * scale
        for nu in range(modes):
            out_ref[nu] = t[:, nu * pair:(nu + 1) * pair]

def couple(hs, l2, pr, pi, kq, bands, zb=16):
    shards = len(hs)
    zblocks, tiles, rows, _ = hs[0].shape
    kq_bands, yc, ng, lanes = kq.shape
    modes = pr.shape[0]
    return pl.pallas_call(
        functools.partial(couple_kernel, shards=shards, yc=yc, bands=bands, modes=modes, zb=zb, scale=float(ng) ** -1.5),
        grid=(ng // zb,),
        in_specs=[pl.BlockSpec((zb // 8, tiles, rows, 128), lambda i: (i, 0, 0, 0))] * shards
        + [pl.BlockSpec(l2.shape, lambda i: (0, 0))]
        + [pl.BlockSpec((modes, yc, zb, lanes), lambda i: (0, 0, i, 0))] * 2
        + [pl.BlockSpec((kq_bands, yc, zb, lanes), lambda i: (0, 0, i, 0))],
        out_specs=pl.BlockSpec((modes, kq_bands, 2 * bands), lambda i: (0, 0, 0)),
        out_shape=jax.ShapeDtypeStruct((modes, kq_bands, 2 * bands), jnp.float32),
        scratch_shapes=[
            pltpu.VMEM((zb, tiles * 128, lanes), jnp.float32),
            pltpu.VMEM((zb // 8, kq_bands * 8, lanes), jnp.float32),
            pltpu.VMEM((kq_bands, zb * lanes), jnp.bfloat16),
            pltpu.VMEM((modes * 2 * bands, zb * lanes), jnp.bfloat16),
            pltpu.VMEM((modes * 2 * bands, kq_bands), jnp.float32),
        ],
        compiler_params=pltpu.CompilerParams(vmem_limit_bytes=60 << 20, dimension_semantics=("arbitrary",)),
        cost_estimate=pl.CostEstimate(flops=4 * bands * modes * kq_bands * yc * ng * lanes, bytes_accessed=kq.size * 2 + shards * hs[0].size * 4, transcendentals=0),
        name="couple",
    )(*hs, l2, pr, pi, kq)


def waves(rows, columns, size):
    angles = (rows[:, None] * columns[None, :] % size).astype(jnp.float32) * (2.0 * math.pi / size)
    return jnp.cos(angles), jnp.sin(angles)


def partner(value, offset, shards):
    return lax.ppermute(value, "pw", [(i, i ^ offset) for i in range(shards)])


def spread(real, imag, cells, shards):
    held = {0: (real, imag)}
    if shards == 8:
        real_x, imag_y = partner(real, 2, 8), partner(imag, 4, 8)
        imag_x, real_y = partner(imag, 2, 8), partner(real, 4, 8)
        held[1] = (partner(real, 1, 8), partner(imag, 1, 8))
        held[2], held[4] = (real_x, imag_x), (real_y, imag_y)
        held[6] = (partner(real_x, 4, 8), partner(imag_y, 2, 8))
        for k in (2, 4, 6):
            held[k + 1] = tuple(partner(part, 1, 8) for part in held[k])
    else:
        for k in range(1, shards):
            held[k] = (partner(real, k, shards), partner(imag, k, shards))
    return [held[k] + (cells if k == 0 else partner(cells, k, shards),) for k in range(shards)]


def on_device(wave_coeffs, sphere_map, wave_kq, potential, shift_map):
    shards, modes = lax.axis_size("pw"), lax.axis_size("mode")
    me, mode_at = lax.axis_index("pw"), lax.axis_index("mode")
    kq_bands, yc, ng, lanes = wave_kq.shape
    bands, planes = wave_coeffs.shape[1], ng // shards
    axis = jnp.arange(ng, dtype=jnp.int32)
    columns = me * yc + jnp.arange(yc, dtype=jnp.int32)

    parts = spread(wave_coeffs[0], wave_coeffs[1], sphere_map[None, :], shards)
    ring = [
        potential if r == 0 else lax.ppermute(potential, "mode", [((i + r) % modes, i) for i in range(modes)])
        for r in range(modes)
    ]
    pot = jnp.concatenate(ring, 0)

    cos_y, sin_y = waves(columns, axis, ng)
    ty = jnp.concatenate([cos_y, sin_y], 0).astype(jnp.bfloat16)
    cos_z, sin_z = waves(axis, axis, ng)
    l1 = jnp.concatenate(
        [jnp.concatenate([cos_z, -sin_z], 1), jnp.concatenate([sin_z, cos_z], 1)], 0
    ).astype(jnp.bfloat16)
    g1 = (me ^ jnp.arange(shards, dtype=jnp.int32))[:, None] * planes + jnp.arange(planes, dtype=jnp.int32)
    cos_x, sin_x = (t.reshape(shards, planes, ng) for t in waves(g1.reshape(-1), axis, ng))
    l2 = (
        jnp.stack([jnp.concatenate([cos_x, sin_x], -1), jnp.concatenate([-sin_x, cos_x], -1)], 1)
        .reshape(2 * ng, 2 * ng)
        .astype(jnp.bfloat16)
    )

    phase_sum = (
        shift_map[0] * axis[None, None, :]
        + shift_map[1] * columns[:, None, None]
        + shift_map[2] * axis[None, :, None]
    ) % ng
    angles = phase_sum.astype(jnp.float32) * (2.0 * math.pi / ng)
    phase_cos, phase_sin = jnp.cos(angles), jnp.sin(angles)
    pot_real = pot[..., :ng].astype(jnp.float32)
    pot_imag = pot[..., ng:].astype(jnp.float32)
    pr = pot_real * phase_cos + pot_imag * phase_sin
    pi = pot_imag * phase_cos - pot_real * phase_sin
    pr, pi = jnp.concatenate([pr, pr], -1), jnp.concatenate([pi, pi], -1)

    hs = [place(re, im, cells, ty, l1, ng=ng, yc=yc, planes=planes) for re, im, cells in parts]
    g = couple(hs, l2, pr, pi, wave_kq, bands)

    g = lax.dynamic_slice_in_dim(jnp.concatenate([g, g], 0), (modes - mode_at) % modes, modes, 0)
    own = kq_bands // shards
    g = g.astype(jnp.bfloat16).reshape(modes, shards, own, 2 * bands).transpose(1, 0, 2, 3)
    g = lax.all_to_all(g.reshape(shards * modes, own, 2 * bands), ("pw", "mode"), 0, 0, tiled=True)
    g = g.reshape(shards, modes, own, 2, bands).astype(jnp.float32).sum(0)
    return g.transpose(1, 2, 0, 3).reshape(own, 2, modes * bands, 1)


def solution(mesh):
    placed = (
        P(None, "mode", "pw"),
        P("pw"),
        P(None, "pw", None, None),
        P("mode", "pw", None, None),
        P(),
    )
    return jax.shard_map(
        on_device,
        mesh=mesh,
        in_specs=placed,
        out_specs=P("pw", None, None, "mode"),
        check_vma=False,
    )
```

```python
import functools
import math

import jax
import jax.numpy as jnp
from jax import lax
from jax.experimental import pallas as pl
from jax.experimental.pallas import tpu as pltpu
from jax.sharding import PartitionSpec as P

NT = (((1,), (1,)), ((), ()))
TN = (((0,), (0,)), ((), ()))


def rows_of(row, count):
    if count % 16:
        return jnp.broadcast_to(row, (count, row.shape[1])).astype(jnp.bfloat16)
    tile = jnp.broadcast_to(row, (16, row.shape[1])).astype(jnp.bfloat16)
    return jnp.concatenate([tile] * (count // 16), 0)


def place_kernel(*refs, ng, yc, planes, chunk):
    *data, map_ref, ty_ref, l1_ref, h_ref, oht, wst, gt = refs
    re_ref, im_ref = data if len(data) == 2 else (data[0].at[0], data[0].at[1])
    bands, slots = re_ref.shape
    half = wst.shape[0] // 2
    rows = planes * ng
    used = yc * bands
    if used < half:
        for c in range(2):
            wst[c * half + used:(c + 1) * half] = jnp.zeros((half - used, slots), jnp.bfloat16)
    for j in range(slots // chunk):
        sl = slice(j * chunk, (j + 1) * chunk)
        cells = map_ref[:, sl]
        key = (cells // (ng * ng)) * ng + cells % ng
        g2 = (cells // ng) % ng
        ohy = (lax.broadcasted_iota(jnp.int32, (ng, chunk), 0) == g2).astype(jnp.bfloat16)
        t = jnp.dot(ty_ref[...], ohy, preferred_element_type=jnp.float32)
        oht[:, sl] = (lax.broadcasted_iota(jnp.int32, (rows, chunk), 0) == key).astype(jnp.bfloat16)
        cr = re_ref[:, sl].astype(jnp.float32)
        ci = im_ref[:, sl].astype(jnp.float32)
        for y in range(yc):
            tr = t[y:y + 1]
            ti = t[yc + y:yc + y + 1]
            wst[y * bands:(y + 1) * bands, sl] = (cr * tr - ci * ti).astype(jnp.bfloat16)
            wst[half + y * bands:half + (y + 1) * bands, sl] = (cr * ti + ci * tr).astype(jnp.bfloat16)
    g = lax.dot_general(oht[...], wst[...], (((1,), (1,)), ((), ())), preferred_element_type=jnp.float32)
    gt[...] = g.astype(jnp.bfloat16)
    for p in range(planes):
        part = jnp.concatenate([gt[p * ng:(p + 1) * ng, :half], gt[p * ng:(p + 1) * ng, half:]], 0)
        res = jnp.dot(l1_ref[...], part, preferred_element_type=jnp.float32)
        for z in range(ng // 8):
            for t in range(half // 128):
                tile = slice(t * 128, (t + 1) * 128)
                h_ref[z, t, p * 8:(p + 1) * 8] = res[z * 8:(z + 1) * 8, tile]
                h_ref[z, t, (planes + p) * 8:(planes + p + 1) * 8] = res[ng + z * 8:ng + (z + 1) * 8, tile]

def place(data, m, ty, l1, *, ng, yc, planes, chunk=512):
    bands, slots = data[0].shape[-2:]
    chunk = min(chunk, slots)
    half = -(-yc * bands // 128) * 128
    return pl.pallas_call(
        functools.partial(place_kernel, ng=ng, yc=yc, planes=planes, chunk=chunk),
        out_shape=jax.ShapeDtypeStruct((ng // 8, half // 128, 16 * planes, 128), jnp.float32),
        scratch_shapes=[pltpu.VMEM((planes * ng, slots), jnp.bfloat16), pltpu.VMEM((2 * half, slots), jnp.bfloat16), pltpu.VMEM((planes * ng, 2 * half), jnp.bfloat16)],
        compiler_params=pltpu.CompilerParams(vmem_limit_bytes=24 << 20),
        cost_estimate=pl.CostEstimate(flops=2 * planes * ng * slots * 2 * yc * bands, bytes_accessed=bands * slots * 4 + planes * ng * 2 * yc * bands * 4, transcendentals=0),
        name="place",
    )(*data, m, ty, l1)

def couple_kernel(*refs, inputs, yc, bands, modes, zb, ng):
    h_refs, pot_refs = refs[:inputs], refs[inputs:inputs + modes]
    at_ref, l2_ref, kq_ref, out_ref, psi, kf, kqs, wst, acc = refs[inputs + modes:]
    kq_bands = kq_ref.shape[0]
    tiles = h_refs[0].shape[1]
    step = pl.program_id(0)

    @pl.when(step == 0)
    def _():
        acc[...] = jnp.zeros_like(acc)

    for z in range(zb):
        s = jnp.concatenate(
            [
                jnp.concatenate([h[z // 8, t, pl.ds(z % 8, h.shape[2] // 8, stride=8), :] for h in h_refs], 0)
                for t in range(tiles)
            ],
            1,
        ).astype(jnp.bfloat16)
        psi[z] = lax.dot_general(s, l2_ref[...], TN, preferred_element_type=jnp.float32).astype(jnp.bfloat16)

    lane = lax.broadcasted_iota(jnp.int32, (zb, 128), 1)
    lower = lane < ng
    z_at = lax.broadcasted_iota(jnp.int32, (zb, 128), 0) + step * zb
    base = at_ref[0] * (lane % ng) + at_ref[2] * z_at
    pair = 2 * bands

    def make(y, slot):
        kv = kq_ref[:, y].astype(jnp.float32).reshape(kq_bands, zb // 8, 8, 128)
        for h in range(zb // 8):
            kf[slot, h] = kv[:, h].reshape(kq_bands * 8, 128)
        angle = ((base + at_ref[1] * (at_ref[3] + y)) & (ng - 1)).astype(jnp.float32) * (2.0 * math.pi / ng)
        cosine, sine = jnp.cos(angle), jnp.sin(angle)
        sine = jnp.where(lower, sine, -sine)
        prs, pis = [], []
        for nu in range(modes):
            pot = pot_refs[nu][0, y].astype(jnp.float32)
            phased = pot * cosine + pltpu.roll(pot, 64, 1) * sine
            other = pltpu.roll(phased, 64, 1)
            prs.append(jnp.where(lower, phased, other))
            pis.append(jnp.where(lower, other, phased))
        for z in range(zb):
            cols = slice(z * 128, (z + 1) * 128)
            kqs[slot, :, cols] = kf[slot, z // 8, pl.ds(z % 8, kq_bands, stride=8), :].astype(jnp.bfloat16)
            a = psi[z, y * bands:(y + 1) * bands, :128]
            b = psi[z, y * bands:(y + 1) * bands, 128:]
            for nu in range(modes):
                pr, pi = rows_of(prs[nu][z:z + 1], bands), rows_of(pis[nu][z:z + 1], bands)
                wst[slot, nu * pair:nu * pair + bands, cols] = a * pr + b * pi
                wst[slot, nu * pair + bands:(nu + 1) * pair, cols] = a * pi - b * pr

    def add(slot):
        acc[...] += lax.dot_general(wst[slot], kqs[slot], NT, preferred_element_type=jnp.float32)

    for y in range(yc):
        make(y, y % 2)
        if y:
            add((y - 1) % 2)
    add((yc - 1) % 2)

    @pl.when(step == pl.num_programs(0) - 1)
    def _():
        t = acc[...].T * (float(ng) ** -1.5)
        for nu in range(modes):
            out_ref[at_ref[4] ^ nu] = t[:, nu * pair:(nu + 1) * pair]


def couple(hs, pots, at, l2, kq, bands, zb=16, limit=40):
    kq_bands, yc, ng, lanes = kq.shape
    modes = len(pots)
    tiles = hs[0].shape[1]
    return pl.pallas_call(
        functools.partial(couple_kernel, inputs=len(hs), yc=yc, bands=bands, modes=modes, zb=zb, ng=ng),
        grid=(ng // zb,),
        in_specs=[pl.BlockSpec((zb // 8, *h.shape[1:]), lambda i: (i, 0, 0, 0)) for h in hs]
        + [pl.BlockSpec((1, yc, zb, lanes), lambda i: (0, 0, i, 0))] * modes
        + [
            pl.BlockSpec(memory_space=pltpu.SMEM),
            pl.BlockSpec(l2.shape, lambda i: (0, 0)),
            pl.BlockSpec((kq_bands, yc, zb, lanes), lambda i: (0, 0, i, 0)),
        ],
        out_specs=pl.BlockSpec((modes, kq_bands, 2 * bands), lambda i: (0, 0, 0)),
        out_shape=jax.ShapeDtypeStruct((modes, kq_bands, 2 * bands), jnp.float32),
        scratch_shapes=[
            pltpu.VMEM((zb, tiles * 128, 256), jnp.bfloat16),
            pltpu.VMEM((2, zb // 8, kq_bands * 8, lanes), jnp.float32),
            pltpu.VMEM((2, kq_bands, zb * lanes), jnp.bfloat16),
            pltpu.VMEM((2, modes * 2 * bands, zb * lanes), jnp.bfloat16),
            pltpu.VMEM((modes * 2 * bands, kq_bands), jnp.float32),
        ],
        compiler_params=pltpu.CompilerParams(vmem_limit_bytes=limit << 20, dimension_semantics=("arbitrary",)),
        cost_estimate=pl.CostEstimate(
            flops=4 * bands * modes * kq_bands * yc * ng * lanes, bytes_accessed=kq.size * 2, transcendentals=0
        ),
        name="couple",
    )(*hs, *pots, at, l2, kq)


def partner(value, offset, shards):
    return lax.ppermute(value, "pw", [(i, i ^ offset) for i in range(shards)])


def spread(coeffs, shards):
    if shards != 8:
        return [(coeffs if k == 0 else partner(coeffs, k, shards),) for k in range(shards)]
    by_x, by_y = partner(coeffs, 2, 8), partner(coeffs, 4, 8)
    by_core = partner(coeffs, 1, 8)
    far = (partner(by_x[0], 4, 8), partner(by_y[1], 2, 8))
    held = [(coeffs,), (by_core,), (by_x,), (partner(by_x, 1, 8),), (by_y,), (partner(by_y, 1, 8),), far]
    return held + [tuple(partner(part, 1, 8) for part in far)]


def cosines(turns, size):
    return jnp.cos((turns % size).astype(jnp.float32) * (2.0 * math.pi / size)).astype(jnp.bfloat16)


def on_device(wave_coeffs, sphere_map, wave_kq, potential, shift_map):
    shards, modes = lax.axis_size("pw"), lax.axis_size("mode")
    me, mode_at = lax.axis_index("pw"), lax.axis_index("mode")
    kq_bands, yc, ng, lanes = wave_kq.shape
    bands, planes = wave_coeffs.shape[1], ng // shards

    maps, step = sphere_map[None, :], 1
    while step < shards:
        maps = jnp.concatenate([maps, partner(maps, step, shards)], 0)
        step *= 2
    data = spread(wave_coeffs, shards)
    pots = [
        potential if r == 0 else lax.ppermute(potential, "mode", [(i, i ^ r) for i in range(modes)])
        for r in range(modes)
    ]

    quarter = ng // 4
    row = jnp.arange(2 * yc, dtype=jnp.int32)[:, None]
    column = jnp.arange(ng, dtype=jnp.int32)[None, :]
    ty = cosines((me * yc + row % yc) * column - quarter * (row // yc), ng)
    row = jnp.arange(2 * ng, dtype=jnp.int32)[:, None]
    column = jnp.arange(2 * ng, dtype=jnp.int32)[None, :]
    l1 = cosines((row % ng) * (column % ng) + quarter * (column // ng - row // ng), ng)
    k, part = row // (2 * planes), row // planes % 2
    column = jnp.arange(4 * ng, dtype=jnp.int32)[None, :]
    g1 = (me ^ k) * planes + row % planes
    lag = column // ng
    lag = jnp.where(lag == 2, -1, jnp.where(lag == 3, 0, lag))
    l2 = cosines(g1 * (column % ng) + quarter * (part - lag), ng)

    hs = [place(data[k], maps[k:k + 1], ty, l1, ng=ng, yc=yc, planes=planes) for k in range(shards)]
    at = jnp.concatenate([shift_map, jnp.stack([me * yc, mode_at]).astype(jnp.int32)])
    g = couple(hs, pots, at, l2, wave_kq, bands)

    own = kq_bands // shards
    g = g.astype(jnp.bfloat16).reshape(modes, shards, own, 2 * bands).transpose(1, 0, 2, 3)
    g = lax.all_to_all(g.reshape(shards * modes, own, 2 * bands), ("pw", "mode"), 0, 0, tiled=True)
    g = g.reshape(shards, modes, own, 2, bands).astype(jnp.float32).sum(0)
    return g.transpose(1, 2, 0, 3).reshape(own, 2, modes * bands, 1)


def solution(mesh):
    placed = (
        P(None, "mode", "pw"),
        P("pw"),
        P(None, "pw", None, None),
        P("mode", "pw", None, None),
        P(),
    )
    return jax.shard_map(
        on_device,
        mesh=mesh,
        in_specs=placed,
        out_specs=P("pw", None, None, "mode"),
        check_vma=False,
    )
```
